32 devices in a mesh: row: 8 (over z, y), col: 4 (over x, core).
Axes of the slice: x: 2, y: 2, z: 4, core: 2. Of those that a mesh axis runs over, the one named last changes fastest.
Arguments:
- act_quant: bfloat16 [512, 8192], P('row', 'col'), may hold values from -127 to 127, as said below
- act_scale: float32 [512], replicated, may hold values from 0.004 to 0.04
- gate_up_quant: bfloat16 [2, 8192, 29568], P(None, 'col', 'row'), may hold values from -127 to 127, as said below
- gate_up_scale: float32 [2, 29568], P(None, 'row'), may hold values from 5e-05 to 0.0005
- down_quant: bfloat16 [29568, 8192], P('row', 'col'), may hold values from -127 to 127, as said below
- down_scale: float32 [8192], P('col'), may hold values from 3e-05 to 0.0003
Outputs:
- mixed_out: bfloat16 [512, 8192], P('row', 'col')
The draws below stay inside these ranges and needn't reach their ends.
Inputs may be any that keep to these rules, and one draw needn't show every extreme that they name: `act_quant`: whole numbers. `gate_up_quant`: whole numbers. `down_quant`: whole numbers.
All inputs are finite; a program needn't handle non-finite values.
Results may differ from the reference program's by a relative error of at most 0.005.
Values may be sent and summed in bfloat16 or wider, within the bound.
A program may use at most 128 MiB of HBM per device.

```python
import math
import jax
import jax.numpy as jnp

D = 8192
FF = 29568
TOK = 512


def integer_levels(key, shape_dims):
    levels = jax.random.randint(key, shape_dims, -127, 128)
    return levels.astype(jnp.float32).astype(jnp.bfloat16)


def draw_act_quant(key, part):
    return integer_levels(jax.random.fold_in(key, 11), (TOK, D))


def draw_gate_up_quant(key, part):
    return integer_levels(jax.random.fold_in(key, 22), (2, D, FF))


def draw_down_quant(key, part):
    return integer_levels(jax.random.fold_in(key, 33), (FF, D))


def steps_of(rng, shape, pieces, least, top_value):
    level = 1.0
    for axis_at, parts in pieces:
        heights = jax.random.uniform(jax.random.fold_in(jax.random.fold_in(rng, 6), axis_at), (parts,), jnp.float32, least / len(pieces), top_value / len(pieces))
        level = level * jnp.repeat(jnp.exp(heights), shape[axis_at] // parts).reshape((-1,) + (1,) * (len(shape) - 1 - axis_at))
    return level


def setup_inputs(seed: int = 0) -> dict:
    keys = jax.random.split(jax.random.key(seed), 7)
    return {
        "act_quant": draw_act_quant(jax.random.fold_in(keys[6], 71), 0),
        "act_scale": jnp.clip(jnp.exp(jax.random.uniform(keys[1], (TOK,), jnp.float32, math.log(0.004), math.log(0.04))), 0.004, 0.04),
        "gate_up_quant": draw_gate_up_quant(jax.random.fold_in(keys[6], 71), 0),
        "gate_up_scale": jnp.clip(jnp.exp(math.log(0.0005) - 2.3025852 * jax.random.uniform(keys[3], (2, FF), jnp.float32) ** steps_of(keys[3], (2, FF), ((1, 8),), -0.2, 0.2)), 4.999999873689376e-05, 0.0005),
        "down_quant": draw_down_quant(jax.random.fold_in(keys[6], 71), 0),
        "down_scale": jnp.clip(jnp.exp(math.log(0.0003) - 2.3025852 * jax.random.uniform(keys[5], (D,), jnp.float32) ** steps_of(keys[5], (D,), ((0, 4),), -0.2, 0.2)), 2.9999999242136255e-05, 0.0003),
    }


def reference(act_quant, act_scale, gate_up_quant, gate_up_scale, down_quant, down_scale):
    gate_acc = jnp.dot(act_quant, gate_up_quant[0], preferred_element_type=jnp.float32)
    up_acc = jnp.dot(act_quant, gate_up_quant[1], preferred_element_type=jnp.float32)
    gate_val = gate_acc * act_scale[:, None] * gate_up_scale[0][None, :]
    up_val = up_acc * act_scale[:, None] * gate_up_scale[1][None, :]
    hidden = (jax.nn.silu(gate_val) * up_val).astype(jnp.bfloat16)
    out_acc = jnp.dot(hidden, down_quant, preferred_element_type=jnp.float32)
    return (out_acc * down_scale[None, :]).astype(jnp.bfloat16)
```

```python
import functools

import jax
import jax.numpy as jnp
from jax import lax
from jax.experimental import pallas as pl
from jax.experimental.pallas import tpu as pltpu
from jax.sharding import PartitionSpec as P

MESH = pl.DeviceIdType.MESH
SUB = 16
TILE = 512
F32, BF16 = jnp.float32, jnp.bfloat16


def for_tiles(width, fn):
    full = width // TILE
    if full:
        def step(j, carry):
            fn(pl.multiple_of(j * TILE, TILE), TILE)
            return carry
        lax.fori_loop(0, full, step, 0)
    if width % TILE:
        fn(full * TILE, width % TILE)


def kernel(K, Rz, Ry, X, act, act_scale, gu_hbm, gu_scale, down_hbm, down_scale, out,
           wgu, wdn, acts, keep, dsend, drecv, xsend, xrecv, hid, opart, ysend, yrecv, zsend, zrecv, zown,
           w_sem, az_s, az_r, ay_s, ay_r, d_s, d_r, x_s, x_r, h_s, h_r, f_s, f_r, y_s, y_r, z_s, z_r, credit):
    R, C = Rz * Ry, X * 2
    Fl, Dl = wgu.shape[1], wgu.shape[2]
    half = R * SUB // 2
    own = R * SUB // C
    nb = R // C
    row, col = lax.axis_index("row"), lax.axis_index("col")
    z, y = row // Ry, lax.rem(row, Ry)
    x, core = col // 2, lax.rem(col, 2)
    pos = core * X + x
    partner = {"row": row, "col": x * 2 + 1 - core}

    def zdev(dz):
        return {"row": lax.rem(z + dz, Rz) * Ry + y, "col": col}

    def ydev(dy):
        return {"row": z * Ry + lax.rem(y + dy, Ry), "col": col}

    def xdev(dx):
        return {"row": row, "col": lax.rem(x + dx, X) * 2 + core}

    def remote(src, dst, s, r, dev):
        return pltpu.make_async_remote_copy(src_ref=src, dst_ref=dst, send_sem=s, recv_sem=r,
                                            device_id=dev, device_id_type=MESH)

    wcopies = []
    cut = Fl // 2 // SUB * SUB
    for g in range(2):
        for h, part in enumerate((pl.ds(0, cut), pl.ds(cut, Fl - cut))):
            wcopies.append(pltpu.make_async_copy(gu_hbm.at[g, part], wgu.at[g, part], w_sem.at[g * 2 + h]))
    dcopy = pltpu.make_async_copy(down_hbm, wdn, w_sem.at[4])
    for c in wcopies:
        c.start()
    dcopy.start()

    barrier = pltpu.get_barrier_semaphore()
    peers = ([zdev(d) for d in range(1, Rz)] + [ydev(d) for d in range(1, Ry)]
             + [xdev(d) for d in range(1, X)] + [partner])
    for p in peers:
        pl.semaphore_signal(barrier, inc=1, device_id=p, device_id_type=MESH)
    pl.semaphore_wait(barrier, len(peers))

    az = [[remote(act.at[pl.ds(k * SUB, SUB)], acts.at[k, z, y], az_s.at[k, d - 1], az_r.at[k, d - 1], zdev(d))
           for d in range(1, Rz)] for k in range(K)]
    ay = [[remote(acts.at[k, :, y], acts.at[k, :, y], ay_s.at[k, d - 1], ay_r.at[k, d - 1], ydev(d))
           for d in range(1, Ry)] for k in range(K)]
    for k in range(K):
        for c in az[k]:
            c.start()
    for k in range(K):
        acts[k, z, y] = act[k * SUB:(k + 1) * SUB, :]

    def forward_acts(k):
        for c in az[k]:
            c.wait_recv()
        for c in ay[k]:
            c.start()

    dd = [remote(dsend, drecv, d_s.at[k], d_r.at[k], partner) for k in range(K)]
    xx = [[remote(xsend.at[k % 2, d - 1], xrecv.at[k, d - 1], x_s.at[k, d - 1], x_r.at[k, d - 1], xdev(d))
           for d in range(1, X)] for k in range(K)]
    hh = [[remote(hid.at[k, pos], hid.at[k, pos], h_s.at[k, d - 1], h_r.at[k, d - 1], xdev(d))
           for d in range(1, X)] for k in range(K)]
    ff = [remote(hid.at[k, pl.ds(core * X, X)], hid.at[k, pl.ds(core * X, X)], f_s.at[k], f_r.at[k], partner)
          for k in range(K)]
    yy = [[remote(ysend.at[k % 2, d - 1], yrecv.at[k, d - 1], y_s.at[k, d - 1], y_r.at[k, d - 1], ydev(d))
           for d in range(1, Ry)] for k in range(K)]
    zz = [[remote(zsend.at[k % 2, d - 1], zrecv.at[k, d - 1], z_s.at[k, d - 1], z_r.at[k, d - 1], zdev(d))
           for d in range(1, Rz)] for k in range(K)]

    def stage_g(k):
        for c in ay[k]:
            c.wait_recv()
        if k + 1 < K:
            forward_acts(k + 1)
        if k == 0:
            for c in wcopies:
                c.wait()
        else:
            dd[k - 1].wait_send()
        blocks = Rz // 2
        for g in range(2):
            def tile(start, size, g=g):
                lhs = jnp.concatenate([
                    acts[k, pl.ds(core * blocks, blocks)].reshape(half, Dl),
                    acts[k, pl.ds((1 - core) * blocks, blocks)].reshape(half, Dl)], axis=0)
                r = lax.dot_general(lhs, wgu[g, pl.ds(start, size), :], (((1,), (1,)), ((), ())),
                                    preferred_element_type=F32)
                keep[k % 2, g, :, pl.ds(start, size)] = r[:half]
                dsend[g, :, pl.ds(start, size)] = r[half:]
            for_tiles(Fl, tile)
        if k >= 1:
            pl.semaphore_wait(credit, 1)
        dd[k].start()

    def stage_x(k):
        dd[k].wait_recv()
        if k >= 2:
            for c in xx[k - 2]:
                c.wait_send()
        for d in range(1, X):
            rows = pl.ds(pl.multiple_of(lax.rem(x + d, X) * own, own), own)
            for g in range(2):
                def tile(start, size, g=g, rows=rows, d=d):
                    cols = pl.ds(start, size)
                    xsend[k % 2, d - 1, g, :, cols] = (keep[k % 2, g, rows, cols] + drecv[g, rows, cols]).astype(BF16)
                for_tiles(Fl, tile)
            xx[k][d - 1].start()
        rows = pl.ds(pl.multiple_of(x * own, own), own)
        for g in range(2):
            def tile(start, size, g=g):
                cols = pl.ds(start, size)
                keep[k % 2, g, rows, cols] = keep[k % 2, g, rows, cols] + drecv[g, rows, cols]
            for_tiles(Fl, tile)
        if k + 1 < K:
            pl.semaphore_signal(credit, inc=1, device_id=partner, device_id_type=MESH)

    def stage_s(k):
        for c in xx[k]:
            c.wait_recv()
        rows = pl.ds(pl.multiple_of(x * own, own), own)
        scale = jnp.concatenate([act_scale[pos * nb + i, k] for i in range(nb)], axis=0)

        def tile(start, size):
            cols = pl.ds(start, size)
            vals = []
            for g in range(2):
                v = keep[k % 2, g, rows, cols]
                for d in range(1, X):
                    v = v + xrecv[k, d - 1, g, :, cols].astype(F32)
                vals.append(v * scale * gu_scale[g:g + 1, cols])
            hid[k, pos, :, cols] = (vals[0] / (1.0 + jnp.exp(-vals[0])) * vals[1]).astype(BF16)
        for_tiles(Fl, tile)
        for c in hh[k]:
            c.start()

    def stage_d(k):
        for c in hh[k]:
            c.wait_recv()
        ff[k].start()
        if k == 0:
            dcopy.wait()
        if k >= 2:
            for c in yy[k - 2]:
                c.wait_send()
        ff[k].wait_recv()

        def tile(start, size):
            r = jnp.dot(hid[k].reshape(R * SUB, Fl), wdn[:, pl.ds(start, size)], preferred_element_type=F32)
            opart[:, :, :, pl.ds(start, size)] = r.reshape(Rz, Ry, SUB, size)
        for_tiles(Dl, tile)
        for d in range(1, Ry):
            ysend[k % 2, d - 1] = opart[:, lax.rem(y + d, Ry)].astype(BF16)
            yy[k][d - 1].start()

    def stage_y(k):
        for c in yy[k]:
            c.wait_recv()
        if k >= 2:
            for c in zz[k - 2]:
                c.wait_send()
        for d in range(1, Rz + 1):
            zt = lax.rem(z + d, Rz)
            v = opart[zt, y]
            for e in range(1, Ry):
                v = v + yrecv[k, e - 1, zt].astype(F32)
            if d < Rz:
                zsend[k % 2, d - 1] = v.astype(BF16)
                zz[k][d - 1].start()
            else:
                zown[k] = v

    def stage_z(k):
        for c in zz[k]:
            c.wait_recv()
        v = zown[k]
        for d in range(1, Rz):
            v = v + zrecv[k, d - 1].astype(F32)
        out[k * SUB:(k + 1) * SUB, :] = (v * down_scale[...]).astype(BF16)

    forward_acts(0)
    for it in range(K + 3):
        if it < K:
            stage_g(it)
            stage_x(it)
        if 0 <= it - 1 < K:
            stage_s(it - 1)
        if 0 <= it - 3 < K:
            stage_y(it - 3)
        if 0 <= it - 2 < K:
            stage_d(it - 2)
    for k in range(K):
        stage_z(k)

    for k in range(K):
        for c in az[k] + ay[k] + hh[k] + [ff[k]]:
            c.wait_send()
    dd[K - 1].wait_send()
    for k in range(max(K - 2, 0), K):
        for c in xx[k] + yy[k] + zz[k]:
            c.wait_send()


def solution(mesh):
    R, C = mesh.shape["row"], mesh.shape["col"]
    X = C // 2
    Ry = max(d for d in range(1, R + 1) if R % d == 0 and d * d <= R)
    Rz = R // Ry

    def body(act, act_scale, gu, gu_scale, down, down_scale):
        tpr, Dl = act.shape
        Fl = gu.shape[2]
        K = tpr // SUB
        T = R * SUB
        own = T // C
        vmem = pl.BlockSpec(memory_space=pltpu.VMEM)
        hbm = pl.BlockSpec(memory_space=pl.ANY)
        dma = pltpu.SemaphoreType.DMA
        scratch = [
            pltpu.VMEM((2, Fl, Dl), BF16),
            pltpu.VMEM((Fl, Dl), BF16),
            pltpu.VMEM((K, Rz, Ry, SUB, Dl), BF16),
            pltpu.VMEM((2, 2, T // 2, Fl), F32),
            pltpu.VMEM((2, T // 2, Fl), F32),
            pltpu.VMEM((2, T // 2, Fl), F32),
            pltpu.VMEM((2, X - 1, 2, own, Fl), BF16),
            pltpu.VMEM((K, X - 1, 2, own, Fl), BF16),
            pltpu.VMEM((K, C, own, Fl), BF16),
            pltpu.VMEM((Rz, Ry, SUB, Dl), F32),
            pltpu.VMEM((2, Ry - 1, Rz, SUB, Dl), BF16),
            pltpu.VMEM((K, Ry - 1, Rz, SUB, Dl), BF16),
            pltpu.VMEM((2, Rz - 1, SUB, Dl), BF16),
            pltpu.VMEM((K, Rz - 1, SUB, Dl), BF16),
            pltpu.VMEM((K, SUB, Dl), F32),
            dma((5,)),
            dma((K, Rz - 1)), dma((K, Rz - 1)),
            dma((K, Ry - 1)), dma((K, Ry - 1)),
            dma((K,)), dma((K,)),
            dma((K, X - 1)), dma((K, X - 1)),
            dma((K, X - 1)), dma((K, X - 1)),
            dma((K,)), dma((K,)),
            dma((K, Ry - 1)), dma((K, Ry - 1)),
            dma((K, Rz - 1)), dma((K, Rz - 1)),
            pltpu.SemaphoreType.REGULAR,
        ]
        return pl.pallas_call(
            functools.partial(kernel, K, Rz, Ry, X),
            out_shape=jax.ShapeDtypeStruct((tpr, Dl), BF16),
            in_specs=[vmem, vmem, hbm, vmem, hbm, vmem],
            out_specs=vmem,
            scratch_shapes=scratch,
            compiler_params=pltpu.CompilerParams(
                collective_id=0, has_side_effects=True, vmem_limit_bytes=67043328
            ),
        )(act, act_scale.reshape(R, K, SUB, 1), jnp.swapaxes(gu, 1, 2), gu_scale, down, down_scale.reshape(1, Dl))

    in_specs = (P("row", "col"), P(), P(None, "col", "row"), P(None, "row"), P("row", "col"), P("col"))
    return jax.shard_map(body, mesh=mesh, in_specs=in_specs, out_specs=P("row", "col"), check_vma=False)
```
